32 devices in a mesh: ep: 8 (over y, x, core), dp: 4 (over z).
Axes of the slice: x: 2, y: 2, z: 4, core: 2. Of those that a mesh axis runs over, the one named last changes fastest.
Arguments:
- master_weights: float32 [8, 1024, 3584], P('ep', 'dp'), may hold values from -6 to 6
- first_moment: float32 [8, 1024, 3584], P('ep', 'dp'), may hold values from -6 to 6
- second_moment: float32 [8, 1024, 3584], P('ep', 'dp'), may hold values from 0.01 to 4
- expert_ids: int32 [8], replicated, may hold values from 0 to 255, as said below
- bucket_offsets: int32 [1024], replicated, may hold values from 0 to 1023, as said below
- writer_rank: int32 [1024], replicated, may hold values from 0 to 3, as said below
Outputs:
- saved: bfloat16 [3, 8, 1024, 3584], P(None, 'ep', 'dp')
The draws below stay inside these ranges and needn't reach their ends.
Inputs may be any that keep to these rules, and one draw needn't show every extreme that they name: `expert_ids`: 8 different global expert numbers. `bucket_offsets`: each saved row named exactly once. `writer_rank`: of the bucket rows held by any one dp index, exactly 1024 // (4 * 4) are written by each dp index.
All inputs are finite; a program needn't handle non-finite values.
Results may differ from the reference program's by a relative error of at most 0.001.
Values may be sent and summed in bfloat16 or wider, within the bound.
A program may use at most 128 MiB of HBM per device.

```python
import math
import jax
import jax.numpy as jnp

ROWS = 1024
COLS = 3584
ALL_EXPERTS = 256
EXPERTS = 8
N_DP = 4


def layout_tables(key):
    shard_rows = ROWS // N_DP
    shuffle = jax.random.permutation(jax.random.fold_in(key, 11), ROWS).astype(jnp.int32)
    pattern = jnp.tile(jnp.arange(N_DP, dtype=jnp.int32), shard_rows // N_DP)
    shard_keys = jax.random.split(jax.random.fold_in(key, 12), N_DP)
    chosen = jax.vmap(lambda single: jax.random.permutation(single, pattern))(shard_keys).reshape(ROWS)
    writers = jnp.zeros((ROWS,), jnp.int32).at[shuffle].set(chosen.astype(jnp.int32))
    return (shuffle, writers)


def draw_expert_ids(key, part):
    return jax.random.permutation(jax.random.fold_in(key, 5), ALL_EXPERTS)[:EXPERTS].astype(jnp.int32)


def draw_bucket_offsets(key, part):
    return layout_tables(key)[0]


def draw_writer_rank(key, part):
    return layout_tables(key)[1]


def level_of(key, dims, cuts, least, high):
    level = 1.0
    for dim, parts in cuts:
        draws = jax.random.uniform(jax.random.fold_in(jax.random.fold_in(key, 6), dim), (parts,), jnp.float32, least / len(cuts), high / len(cuts))
        level = level * jnp.repeat(jnp.exp(draws), dims[dim] // parts).reshape((-1,) + (1,) * (len(dims) - 1 - dim))
    return level


def scatter_about(own_key, dims, spread, limit, shards=(), kind=jnp.bfloat16):
    drawn = spread * jax.random.normal(own_key, dims, jnp.float32)
    if shards:
        drawn = drawn * level_of(own_key, dims, shards, -0.22, 0.18)
    return jnp.clip(drawn, -limit, limit).astype(kind)


def setup_inputs(seed: int = 0) -> dict:
    streams_of = jax.random.split(jax.random.key(seed), 7)
    master_weights = scatter_about(streams_of[0], (EXPERTS, ROWS, COLS), 1.0, 6.0, ((0, 8), (1, 4)), jnp.float32)
    first_moment = scatter_about(streams_of[1], (EXPERTS, ROWS, COLS), 1.0, 6.0, ((0, 8), (1, 4)), jnp.float32)
    second_moment = jnp.clip(jnp.exp(math.log(4.0) - 5.9914646 * jax.random.uniform(streams_of[2], (EXPERTS, ROWS, COLS), jnp.float32) ** level_of(streams_of[2], (EXPERTS, ROWS, COLS), ((0, 8), (1, 4)), -0.2, 0.2)), 0.01, 4.0)
    expert_ids = draw_expert_ids(jax.random.fold_in(streams_of[6], 71), 0)
    bucket_offsets = draw_bucket_offsets(jax.random.fold_in(streams_of[6], 71), 0)
    writer_rank = draw_writer_rank(jax.random.fold_in(streams_of[6], 71), 0)
    return {"master_weights": master_weights, "first_moment": first_moment, "second_moment": second_moment, "expert_ids": expert_ids, "bucket_offsets": bucket_offsets, "writer_rank": writer_rank}


def destinations(bucket_offsets, writer_rank, shard_rows, groups):
    indicator = (writer_rank[:, None] == jnp.arange(groups, dtype=jnp.int32)[None, :]).astype(jnp.int32)
    before = jnp.cumsum(indicator, axis=0) - indicator
    within = jnp.sum(before * indicator, axis=1).astype(jnp.int32)
    placed = writer_rank * shard_rows + within
    return jnp.take(placed, bucket_offsets)


def reference(master_weights, first_moment, second_moment, expert_ids, bucket_offsets, writer_rank):
    target = destinations(bucket_offsets, writer_rank, ROWS // N_DP, N_DP)
    source_rows = jnp.argsort(target)
    source_order = jnp.argsort(expert_ids)

    def arrange(field):
        moved = jnp.take(field.astype(jnp.bfloat16), source_order, axis=0)
        return jnp.take(moved, source_rows, axis=1)

    return jnp.stack([arrange(master_weights), arrange(first_moment), arrange(second_moment)])
```

```python
import functools
import math

import jax
import jax.numpy as jnp
from jax import lax
from jax.experimental import pallas as pl
from jax.experimental.pallas import tpu as pltpu
from jax.sharding import PartitionSpec as P

MESH = pl.DeviceIdType.MESH
FIELDS = 3


def tables(bucket_offsets, writer_rank, mine, groups):
    total = bucket_offsets.shape[0]
    shard = total // groups
    pair = shard // groups
    p = jnp.arange(total, dtype=jnp.int32)
    q = jnp.arange(shard, dtype=jnp.int32)
    earlier = (writer_rank[None, :] == writer_rank[:, None]) & (p[None, :] < p[:, None])
    place = writer_rank * shard + jnp.sum(earlier.astype(jnp.int32), axis=1)
    target = jnp.sum(jnp.where(bucket_offsets[:, None] == p[None, :], place[None, :], 0), axis=1)
    dest = (target // shard).reshape(groups, shard)
    ahead = (dest[:, None, :] == dest[:, :, None]) & (q[None, None, :] < q[None, :, None])
    rank = jnp.sum(ahead.astype(jnp.int32), axis=2)
    position = lax.dynamic_index_in_dim(dest * pair + rank, mine, 0)
    arrives = jnp.arange(groups, dtype=jnp.int32)[:, None] * pair + rank
    return position, target.reshape(1, total), arrives.reshape(1, total)


def order_of(expert_ids):
    count = expert_ids.shape[0]
    k = jnp.arange(count, dtype=jnp.int32)
    rank = jnp.sum((expert_ids[None, :] < expert_ids[:, None]).astype(jnp.int32), axis=1)
    return jnp.sum(jnp.where(rank[None, :] == k[:, None], k[None, :], 0), axis=1)


def one_hot(index_ref, first, depth):
    rows = lax.broadcasted_iota(jnp.int32, (depth, index_ref.shape[1]), 0) + first
    return (index_ref[...] == rows).astype(jnp.float32).astype(jnp.bfloat16)


def rounded_dot(left, right):
    return jnp.dot(left, right, preferred_element_type=jnp.float32).astype(jnp.bfloat16)


def column_tiles(cols, body):
    tile = cols // 2 if cols % 256 == 0 else cols

    @pl.loop(0, cols // tile)
    def _(i):
        body(pl.ds(pl.multiple_of(i * tile, tile), tile))


def partner(me, offset, n):
    out, bit = 0, 1
    while bit < n:
        out = out + ((me // bit + (offset // bit) % 2) % 2) * bit
        bit *= 2
    return out


def exchange_kernel(n_ep, n_dp, half, *refs_in):
    order_ref, position_ref, target_ref, arrives_ref = refs_in[:4]
    fields_in, out_ref, scratch = refs_in[4 : 4 + FIELDS], refs_in[4 + FIELDS], refs_in[5 + FIELDS :]
    e1 = scratch[: 2 * FIELDS]
    wide, ready, sel, mid, placed, late, before, after = scratch[2 * FIELDS : 2 * FIELDS + 8]
    load, z_send, z_recv, a_send, a_recv, b_send, b_recv, store = scratch[2 * FIELDS + 8 :]
    ep, dp = lax.axis_index("ep"), lax.axis_index("dp")
    _, blocks, depth, cols = out_ref.shape
    rows = blocks * depth
    aligned = depth % 16 == 0
    m_ep, m_dp = blocks // n_ep, blocks // n_dp
    z_order = sorted(range(1, n_dp), key=lambda o: -o)
    e_order = sorted(range(1, n_ep), key=lambda o: (o == 1, o % 2, -o))
    first = pl.ds(0, half)
    last = pl.ds(half, cols - half)

    def span(c):
        return first if c < FIELDS else last

    def load_copy(c):
        return pltpu.make_async_copy(fields_in[c % FIELDS].at[:, span(c)], wide.at[c], load.at[c])

    turns = [c for f in range(FIELDS) for c in (f, FIELDS + f)]
    for c in turns:
        load_copy(c).start()

    barrier = pltpu.get_barrier_semaphore()
    for o in range(1, n_dp):
        pl.semaphore_signal(barrier, inc=1, device_id={"dp": partner(dp, o, n_dp)}, device_id_type=MESH)
    for o in range(1, n_ep):
        pl.semaphore_signal(barrier, inc=1, device_id={"ep": partner(ep, o, n_ep)}, device_id_type=MESH)

    def remote(src, dst, send, recv, axis, peer):
        return pltpu.make_async_remote_copy(
            src_ref=src, dst_ref=dst, send_sem=send, recv_sem=recv,
            device_id={axis: peer}, device_id_type=MESH,
        )

    def z_refs(c):
        return (ready.at[c], mid.at[c]) if c < FIELDS else (mid.at[c], late.at[c - FIELDS])

    def a_ref(c):
        return placed.at[c] if c < FIELDS else ready.at[c]

    def b_ref(c):
        return out_ref.at[c, :, :, first] if c < FIELDS else mid.at[c]

    def z_copies(c):
        src, dst = z_refs(c)
        return [
            remote(
                src.at[pl.ds(partner(dp, o, n_dp) * m_dp, m_dp)], dst.at[pl.ds(dp * m_dp, m_dp)],
                z_send.at[c, o], z_recv.at[c, o], "dp", partner(dp, o, n_dp),
            )
            for o in z_order
        ]

    def a_copies(c):
        return [
            remote(
                a_ref(c).at[pl.ds(partner(ep, o, n_ep) * m_ep, m_ep)], e1[c].at[ep],
                a_send.at[c, o], a_recv.at[c, o], "ep", partner(ep, o, n_ep),
            )
            for o in e_order
        ]

    def b_copies(c):
        return [
            remote(
                sel.at[c, partner(ep, o, n_ep)], b_ref(c).at[pl.ds(ep * m_ep, m_ep)],
                b_send.at[c, o], b_recv.at[c, o], "ep", partner(ep, o, n_ep),
            )
            for o in e_order
        ]

    def start(copies):
        for copy in copies:
            copy.start()

    def arrive(copies):
        for copy in copies:
            copy.wait_recv()

    def own_out(c):
        out_ref[c, pl.ds(ep * m_ep, m_ep), :, first] = sel[c, ep]

    def placed_out(c):
        out_ref[c - FIELDS, :, :, last] = placed[c]

    def sort(c):
        load_copy(c).wait()

        def body(part):
            x = wide[c, :, part].astype(jnp.bfloat16)
            if aligned:
                ready[c, :, :, part] = rounded_dot(before[...], x).reshape(blocks, depth, x.shape[1])
            else:
                @pl.loop(0, blocks)
                def _(i):
                    ready[c, i, :, part] = rounded_dot(one_hot(position_ref, i * depth, depth), x)

        column_tiles(half, body)

    def place(c, src):
        def body(part):
            if aligned:
                x = src[:, :, part].reshape(rows, part.size)
                placed[c, :, :, part] = rounded_dot(after[...], x).reshape(blocks, depth, part.size)
            else:
                @pl.loop(0, blocks)
                def _(i):
                    def add(j, total):
                        return total + jnp.dot(
                            after[i, j], src[j, :, part], preferred_element_type=jnp.float32
                        )

                    total = lax.fori_loop(0, blocks, add, jnp.zeros((depth, part.size), jnp.float32))
                    placed[c, i, :, part] = total.astype(jnp.bfloat16)

        column_tiles(half, body)

    def after_of(i, j, size):
        return lax.dot_general(
            one_hot(target_ref, dp * rows + i * size, size), one_hot(arrives_ref, j * size, size),
            (((1,), (1,)), ((), ())), preferred_element_type=jnp.float32,
        ).astype(jnp.bfloat16)

    def z_start(c):
        start(z_copies(c))
        src, dst = z_refs(c)
        own = pl.ds(dp * m_dp, m_dp)
        dst[own] = src[own]

    def a_start(c):
        start(a_copies(c))
        e1[c][ep] = a_ref(c)[pl.ds(ep * m_ep, m_ep)]

    def a_to_b(c):
        arrive(a_copies(c))
        for k in range(n_ep):
            sel[c, k] = e1[c][order_ref[k]]
        start(b_copies(c))
        if c < FIELDS:
            own_out(c)
        else:
            mid[c, pl.ds(ep * m_ep, m_ep)] = sel[c, ep]

    def z_to_a(c):
        arrive(z_copies(c))
        place(c, mid.at[c])
        a_start(c)

    def b_to_z(c):
        arrive(b_copies(c))
        z_start(c)

    def finish(c):
        arrive(z_copies(c))
        place(c, late.at[c - FIELDS])
        placed_out(c)

    if aligned:
        before[...] = one_hot(position_ref, 0, rows)
    for c in turns:
        sort(c)
        if c == 0:
            pl.semaphore_wait(barrier, n_dp + n_ep - 2)
        (z_start if c < FIELDS else a_start)(c)
    if aligned:
        after[...] = after_of(0, 0, rows)
    else:
        @pl.loop(0, blocks)
        def _(i):
            @pl.loop(0, blocks)
            def _(j):
                after[i, j] = after_of(i, j, depth)
    a_to_b(3)
    a_to_b(4)
    z_to_a(0)
    a_to_b(5)
    b_to_z(3)
    z_to_a(1)
    b_to_z(4)
    a_to_b(0)
    z_to_a(2)
    b_to_z(5)
    finish(3)
    a_to_b(1)
    a_to_b(2)
    finish(4)
    for c in range(FIELDS):
        arrive(b_copies(c))
    finish(5)
    for c in range(2 * FIELDS):
        for copies in (z_copies(c), a_copies(c), b_copies(c)):
            for copy in copies:
                copy.wait_send()


def exchange(order, indices, arrays, n_ep, n_dp):
    rows, cols = arrays[0].shape
    depth = math.gcd(rows // n_dp, rows // n_ep)
    blocks = rows // depth
    half = cols // 2
    per = blocks // n_ep
    chunks = 2 * FIELDS
    bf16, dma = jnp.bfloat16, pltpu.SemaphoreType.DMA
    vmem = pl.BlockSpec(memory_space=pltpu.VMEM)
    anywhere = pl.BlockSpec(memory_space=pl.ANY)
    square = (rows, rows) if depth % 16 == 0 else (blocks, blocks, depth, depth)
    return pl.pallas_call(
        functools.partial(exchange_kernel, n_ep, n_dp, half),
        out_shape=pltpu.VMEM((FIELDS, blocks, depth, cols), bf16),
        in_specs=[pl.BlockSpec(memory_space=pltpu.SMEM), vmem, vmem, vmem] + [anywhere] * FIELDS,
        out_specs=vmem,
        scratch_shapes=[pltpu.VMEM((n_ep, per, depth, half), bf16)] * chunks
        + [
            pltpu.VMEM((chunks, rows, half), jnp.float32),
            pltpu.VMEM((chunks, blocks, depth, half), bf16),
            pltpu.VMEM((chunks, n_ep, per, depth, half), bf16),
            pltpu.VMEM((chunks, blocks, depth, half), bf16),
            pltpu.VMEM((chunks, blocks, depth, half), bf16),
            pltpu.VMEM((FIELDS, blocks, depth, half), bf16),
            pltpu.VMEM(square, bf16),
            pltpu.VMEM(square, bf16),
            dma((chunks,)),
            dma((chunks, n_dp)),
            dma((chunks, n_dp)),
            dma((chunks, n_ep)),
            dma((chunks, n_ep)),
            dma((chunks, n_ep)),
            dma((chunks, n_ep)),
            dma((chunks,)),
        ],
        compiler_params=pltpu.CompilerParams(collective_id=0, has_side_effects=True, vmem_limit_bytes=54 * 2**20),
    )(order, *indices, *arrays)


def on_device(master_weights, first_moment, second_moment, expert_ids, bucket_offsets, writer_rank):
    n_dp, n_ep = lax.axis_size("dp"), lax.axis_size("ep")
    _, rows, cols = master_weights.shape
    indices = tables(bucket_offsets, writer_rank, lax.axis_index("dp"), n_dp)
    arrays = (master_weights[0], first_moment[0], second_moment[0])
    saved = exchange(order_of(expert_ids), indices, arrays, n_ep, n_dp)
    return saved.reshape(FIELDS, 1, rows, cols)


def solution(mesh):
    return jax.shard_map(
        on_device,
        mesh=mesh,
        in_specs=(P("ep", "dp", None), P("ep", "dp", None), P("ep", "dp", None), P(), P(), P()),
        out_specs=P(None, "ep", "dp", None),
        check_vma=False,
    )
```

```python
import functools
import math

import jax
import jax.numpy as jnp
from jax import lax
from jax.experimental import pallas as pl
from jax.experimental.pallas import tpu as pltpu
from jax.sharding import PartitionSpec as P

MESH = pl.DeviceIdType.MESH
FIELDS = 3
PACK = 16
BF16, F32, I32 = jnp.bfloat16, jnp.float32, jnp.int32


def cut(total, parts):
    units = total // 128
    return 128 * min(max(round(units * parts), 1), units - 1)


def widths(cols):
    if cols % 128:
        return [cols // 2] * FIELDS
    return [cut(cols, 2 / 7), cut(cols, 1 / 2), cut(cols, 5 / 7)]


def as_bf16(mask):
    return mask.astype(F32).astype(BF16)


def dot(left, right):
    return jnp.dot(left, right, preferred_element_type=F32)


def iota(shape, axis):
    return lax.broadcasted_iota(I32, shape, axis)


def one_hot(index_ref, first, depth):
    return as_bf16(index_ref[...] == iota((depth, index_ref.shape[1]), 0) + first)


def row_of(stack, row):
    return jnp.sum(jnp.where(iota(stack.shape, 0) == row, stack, 0.0), axis=0, keepdims=True)


def stack_rows(rows, width):
    out = jnp.zeros((PACK, width), F32)
    for i, row in enumerate(rows):
        out = jnp.where(iota((PACK, width), 0) == i, row, out)
    return out.astype(BF16)


def column_tiles(cols, body):
    tile = next((t for t in (512, 256, 128) if cols % t == 0), cols)

    @pl.loop(0, cols // tile)
    def _(i):
        body(pl.ds(pl.multiple_of(i * tile, tile), tile))


def partner(me, offset, n):
    out, bit = 0, 1
    while bit < n:
        out = out + ((me // bit + (offset // bit) % 2) % 2) * bit
        bit *= 2
    return out


def exchange_kernel(n_ep, n_dp, split, *refs_in):
    ids_ref, offsets_ref, writers_ref = refs_in[:3]
    fields_in, out_ref, scratch = refs_in[3 : 3 + FIELDS], refs_in[3 + FIELDS], list(refs_in[4 + FIELDS :])

    def take(count):
        head = scratch[:count]
        del scratch[:count]
        return head

    chunks = 2 * FIELDS
    wide, ready, mid, e1, sel = (take(chunks) for _ in range(5))
    placed, early, late = take(FIELDS), take(FIELDS), take(FIELDS)
    order_ref, position_ref, target_ref, arrives_ref, before, after, ahead = take(7)
    load, z_send, z_recv, a_send, a_recv, b_send, b_recv = scratch
    ep, dp = lax.axis_index("ep"), lax.axis_index("dp")
    _, blocks, depth, cols = out_ref.shape
    rows = blocks * depth
    total = offsets_ref.shape[1]
    pair = rows // n_dp
    aligned = depth % PACK == 0
    m_ep, m_dp = blocks // n_ep, blocks // n_dp
    z_order = sorted(range(1, n_dp), key=lambda o: (o == 1, o))
    e_order = sorted(range(1, n_ep), key=lambda o: (o == 1, o % 2, -o))

    def span(c):
        f = c % FIELDS
        return pl.ds(0, split[f]) if c < FIELDS else pl.ds(split[f], cols - split[f])

    def load_copy(c):
        return pltpu.make_async_copy(fields_in[c % FIELDS].at[:, span(c)], wide[c], load.at[c])

    turns = [c for f in range(FIELDS) for c in (f, FIELDS + f)]
    for c in turns:
        load_copy(c).start()

    barrier = pltpu.get_barrier_semaphore()
    for o in range(1, n_dp):
        pl.semaphore_signal(barrier, inc=1, device_id={"dp": partner(dp, o, n_dp)}, device_id_type=MESH)
    for o in range(1, n_ep):
        pl.semaphore_signal(barrier, inc=1, device_id={"ep": partner(ep, o, n_ep)}, device_id_type=MESH)

    def remote(src, dst, send, recv, axis, peer):
        return pltpu.make_async_remote_copy(
            src_ref=src, dst_ref=dst, send_sem=send, recv_sem=recv,
            device_id={axis: peer}, device_id_type=MESH,
        )

    def z_refs(c):
        return (ready[c], mid[c]) if c < FIELDS else (early[c - FIELDS], late[c - FIELDS])

    def a_ref(c):
        return placed[c] if c < FIELDS else ready[c]

    def b_ref(c):
        return out_ref.at[c, :, :, span(c)] if c < FIELDS else mid[c]

    def z_copies(c):
        src, dst = z_refs(c)
        return [
            remote(
                src.at[pl.ds(partner(dp, o, n_dp) * m_dp, m_dp)], dst.at[pl.ds(dp * m_dp, m_dp)],
                z_send.at[c, o], z_recv.at[c, o], "dp", partner(dp, o, n_dp),
            )
            for o in z_order
        ]

    def a_copies(c):
        return [
            remote(
                a_ref(c).at[pl.ds(partner(ep, o, n_ep) * m_ep, m_ep)], e1[c].at[ep],
                a_send.at[c, o], a_recv.at[c, o], "ep", partner(ep, o, n_ep),
            )
            for o in e_order
        ]

    def b_copies(c):
        return [
            remote(
                sel[c].at[partner(ep, o, n_ep)], b_ref(c).at[pl.ds(ep * m_ep, m_ep)],
                b_send.at[c, o], b_recv.at[c, o], "ep", partner(ep, o, n_ep),
            )
            for o in e_order
        ]

    def start(copies):
        for copy in copies:
            copy.start()

    def arrive(copies):
        for copy in copies:
            copy.wait_recv()

    def make_order():
        @pl.loop(0, n_ep)
        def _(k):
            def rank_of(e):
                def count(f, rank):
                    tied = (ids_ref[f] == ids_ref[e]) & (f < e)
                    return rank + ((ids_ref[f] < ids_ref[e]) | tied).astype(I32)

                return lax.fori_loop(0, n_ep, count, jnp.int32(0))

            order_ref[k] = lax.fori_loop(
                0, n_ep, lambda e, r: r + jnp.where(rank_of(e) == k, e, 0), jnp.int32(0)
            )

    def groups_of(writer):
        return (writer == iota((PACK, writer.shape[1]), 0).astype(writer.dtype)).astype(F32)

    def rank_in(groups):
        return dot(groups.astype(BF16), ahead[...])

    def pick(table, s):
        offsets = offsets_ref[:, pl.ds(pl.multiple_of(s * rows, rows), rows)]
        return dot(table, as_bf16(offsets == iota((total, rows), 0)))

    def writer_and_rank(writer):
        groups = groups_of(writer)
        return jnp.sum(groups * rank_in(groups), axis=0, keepdims=True)

    def make_position():
        ahead[...] = as_bf16(iota((rows, rows), 0) < iota((rows, rows), 1))
        picked = pick(stack_rows([writers_ref[...].astype(F32)], total), dp)
        writer = row_of(picked, 0)
        position_ref[...] = (writer * pair + writer_and_rank(writer)).astype(I32)

    def make_targets():
        carry = jnp.zeros((PACK, 1), F32)
        within = []
        for s in range(n_dp):
            groups = groups_of(writers_ref[:, s * rows : (s + 1) * rows])
            count = rank_in(groups) + carry
            carry = carry + jnp.sum(groups, axis=1, keepdims=True)
            within.append(jnp.sum(groups * count, axis=0, keepdims=True).astype(I32))
        place = jnp.concatenate(within, axis=1)
        table = stack_rows(
            [writers_ref[...].astype(F32), (place // 256).astype(F32), (place % 256).astype(F32)], total
        )

        @pl.loop(0, n_dp)
        def _(s):
            picked = pick(table, s)
            writer = row_of(picked, 0)
            here = pl.ds(pl.multiple_of(s * rows, rows), rows)
            target_ref[:, here] = (writer * rows + row_of(picked, 1) * 256 + row_of(picked, 2)).astype(I32)
            arrives_ref[:, here] = (writer_and_rank(writer)).astype(I32) + s * pair

    def after_of(i, j, size):
        return lax.dot_general(
            one_hot(target_ref, dp * rows + i * size, size), one_hot(arrives_ref, j * size, size),
            (((1,), (1,)), ((), ())), preferred_element_type=F32,
        ).astype(BF16)

    def permute(matrix, src, dst):
        def body(part):
            if aligned:
                x = src[:, :, part].reshape(rows, part.size)
                dst[:, :, part] = dot(matrix[...], x).astype(BF16).reshape(blocks, depth, part.size)
            else:
                @pl.loop(0, blocks)
                def _(i):
                    def add(j, so_far):
                        return so_far + dot(matrix[i, j], src[j, :, part])

                    dst[i, :, part] = lax.fori_loop(
                        0, blocks, add, jnp.zeros((depth, part.size), F32)
                    ).astype(BF16)

        column_tiles(dst.shape[2], body)

    def sort(c):
        load_copy(c).wait()

        def body(part):
            x = wide[c][:, part].astype(BF16)
            if aligned:
                ready[c][:, :, part] = dot(before[...], x).astype(BF16).reshape(blocks, depth, part.size)
            else:
                @pl.loop(0, blocks)
                def _(i):
                    ready[c][i, :, part] = dot(one_hot(position_ref, i * depth, depth), x).astype(BF16)

        column_tiles(ready[c].shape[2], body)

    def narrow(c):
        load_copy(c).wait()

        def body(part):
            x = wide[c][:, part].astype(BF16)
            if aligned:
                ready[c][:, :, part] = x.reshape(blocks, depth, part.size)
            else:
                @pl.loop(0, blocks)
                def _(i):
                    keep = as_bf16(iota((depth, rows), 0) + i * depth == iota((depth, rows), 1))
                    ready[c][i, :, part] = dot(keep, x).astype(BF16)

        column_tiles(ready[c].shape[2], body)

    def z_start(c):
        start(z_copies(c))
        src, dst = z_refs(c)
        own = pl.ds(dp * m_dp, m_dp)
        dst[own] = src[own]

    def a_start(c):
        start(a_copies(c))
        e1[c][ep] = a_ref(c)[pl.ds(ep * m_ep, m_ep)]

    def a_to_b(c):
        arrive(a_copies(c))
        for k in range(n_ep):
            sel[c][k] = e1[c][order_ref[k]]
        start(b_copies(c))
        b_ref(c)[pl.ds(ep * m_ep, m_ep)] = sel[c][ep]

    def z_to_a(c):
        arrive(z_copies(c))
        permute(after, mid[c], placed[c])
        a_start(c)

    def b_to_z(c):
        arrive(b_copies(c))
        permute(before, mid[c], early[c - FIELDS])
        z_start(c)

    def finish(c):
        arrive(z_copies(c))
        permute(after, late[c - FIELDS], out_ref.at[c - FIELDS, :, :, span(c)])

    make_position()
    if aligned:
        before[...] = one_hot(position_ref, 0, rows)
    sort(0)
    pl.semaphore_wait(barrier, n_dp + n_ep - 2)
    z_start(0)
    narrow(3)
    a_start(3)
    for f in range(1, FIELDS):
        sort(f)
        z_start(f)
        narrow(FIELDS + f)
        a_start(FIELDS + f)
    make_order()
    make_targets()
    if aligned:
        after[...] = after_of(0, 0, rows)
    else:
        @pl.loop(0, blocks)
        def _(i):
            @pl.loop(0, blocks)
            def _(j):
                after[i, j] = after_of(i, j, depth)
                mine = as_bf16(position_ref[...] == iota((depth, rows), 0) + i * depth)
                whose = as_bf16(iota((depth, rows), 1) == iota((depth, rows), 0) + j * depth)
                before[i, j] = lax.dot_general(
                    mine, whose, (((1,), (1,)), ((), ())), preferred_element_type=F32
                ).astype(BF16)
    z_to_a(0)
    a_to_b(3)
    a_to_b(4)
    a_to_b(5)
    z_to_a(1)
    a_to_b(0)
    b_to_z(3)
    z_to_a(2)
    b_to_z(4)
    b_to_z(5)
    a_to_b(1)
    finish(3)
    a_to_b(2)
    finish(4)
    arrive(b_copies(0))
    arrive(b_copies(1))
    finish(5)
    arrive(b_copies(2))
    for c in range(chunks):
        for copies in (z_copies(c), a_copies(c), b_copies(c)):
            for copy in copies:
                copy.wait_send()


def exchange(expert_ids, offsets, writers, arrays, n_ep, n_dp):
    rows, cols = arrays[0].shape
    total = offsets.shape[1]
    depth = math.gcd(rows // n_dp, rows // n_ep)
    blocks = rows // depth
    split = widths(cols)
    per = blocks // n_ep
    size = split + [cols - w for w in split]
    dma = pltpu.SemaphoreType.DMA
    vmem = pl.BlockSpec(memory_space=pltpu.VMEM)
    square = (rows, rows) if depth % PACK == 0 else (blocks, blocks, depth, depth)

    def each(shape, widths_of, kind=BF16):
        return [pltpu.VMEM((*shape, w), kind) for w in widths_of]

    first, last = size[:FIELDS], size[FIELDS:]
    chunks = 2 * FIELDS
    return pl.pallas_call(
        functools.partial(exchange_kernel, n_ep, n_dp, split),
        out_shape=pltpu.VMEM((FIELDS, blocks, depth, cols), BF16),
        in_specs=[pl.BlockSpec(memory_space=pltpu.SMEM), vmem, vmem] + [pl.BlockSpec(memory_space=pl.ANY)] * FIELDS,
        out_specs=vmem,
        scratch_shapes=each((rows,), size, F32)
        + each((blocks, depth), size)
        + each((blocks, depth), size)
        + each((n_ep, per, depth), size)
        + each((n_ep, per, depth), size)
        + each((blocks, depth), first)
        + each((blocks, depth), last)
        + each((blocks, depth), last)
        + [
            pltpu.SMEM((n_ep,), I32),
            pltpu.VMEM((1, rows), I32),
            pltpu.VMEM((1, total), I32),
            pltpu.VMEM((1, total), I32),
            pltpu.VMEM(square, BF16),
            pltpu.VMEM(square, BF16),
            pltpu.VMEM((rows, rows), BF16),
            dma((chunks,)),
            dma((chunks, n_dp)),
            dma((chunks, n_dp)),
            dma((chunks, n_ep)),
            dma((chunks, n_ep)),
            dma((chunks, n_ep)),
            dma((chunks, n_ep)),
        ],
        compiler_params=pltpu.CompilerParams(
            collective_id=0, has_side_effects=True, vmem_limit_bytes=54 * 2**20
        ),
    )(expert_ids, offsets, writers, *arrays)


def on_device(master_weights, first_moment, second_moment, expert_ids, bucket_offsets, writer_rank):
    n_dp, n_ep = lax.axis_size("dp"), lax.axis_size("ep")
    _, rows, cols = master_weights.shape
    total = bucket_offsets.shape[0]
    arrays = (master_weights[0], first_moment[0], second_moment[0])
    saved = exchange(
        expert_ids, bucket_offsets.reshape(1, total), writer_rank.reshape(1, total), arrays, n_ep, n_dp
    )
    return saved.reshape(FIELDS, 1, rows, cols)


def solution(mesh):
    return jax.shard_map(
        on_device,
        mesh=mesh,
        in_specs=(P("ep", "dp", None), P("ep", "dp", None), P("ep", "dp", None), P(), P(), P()),
        out_specs=P(None, "ep", "dp", None),
        check_vma=False,
    )
```

```python
import functools
import math

import jax
import jax.numpy as jnp
from jax import lax
from jax.experimental import pallas as pl
from jax.experimental.pallas import tpu as pltpu
from jax.sharding import PartitionSpec as P

MESH = pl.DeviceIdType.MESH
FIELDS = 3
PACK = 16
BF16, F32, I32 = jnp.bfloat16, jnp.float32, jnp.int32


def cut(total, parts):
    units = total // 128
    return 128 * min(max(round(units * parts), 1), units - 1)


def widths(cols):
    if cols % 128:
        return [cols // 2] * FIELDS
    return [cut(cols, 2 / 7), cut(cols, 1 / 2), cut(cols, 5 / 7)]


def as_bf16(mask):
    return mask.astype(F32).astype(BF16)


def dot(left, right):
    return jnp.dot(left, right, preferred_element_type=F32)


def iota(shape, axis):
    return lax.broadcasted_iota(I32, shape, axis)


def one_hot(index_ref, first, depth):
    return as_bf16(index_ref[...] == iota((depth, index_ref.shape[1]), 0) + first)


def row_of(stack, row):
    return jnp.sum(jnp.where(iota(stack.shape, 0) == row, stack, 0.0), axis=0, keepdims=True)


def stack_rows(rows, width):
    out = jnp.zeros((PACK, width), F32)
    for i, row in enumerate(rows):
        out = jnp.where(iota((PACK, width), 0) == i, row, out)
    return out.astype(BF16)


def column_tiles(cols, body):
    tile = next((t for t in (512, 256, 128) if cols % t == 0), cols)

    @pl.loop(0, cols // tile)
    def _(i):
        body(pl.ds(pl.multiple_of(i * tile, tile), tile))


def partner(me, offset, n):
    out, bit = 0, 1
    while bit < n:
        out = out + ((me // bit + (offset // bit) % 2) % 2) * bit
        bit *= 2
    return out


def exchange_kernel(n_ep, n_dp, split, *refs_in):
    indices_in = refs_in[:3]
    fields_in, out_ref, scratch = refs_in[3 : 3 + FIELDS], refs_in[3 + FIELDS], list(refs_in[4 + FIELDS :])

    def take(count):
        head = scratch[:count]
        del scratch[:count]
        return head

    chunks = 2 * FIELDS
    wide, ready, mid, e1, sel = (take(chunks) for _ in range(5))
    placed, early, late = take(FIELDS), take(FIELDS), take(FIELDS)
    ids_ref, offsets_ref, writers_ref = take(3)
    rank_ref, order_ref, position_ref, target_ref, arrives_ref, before, after, ahead = take(8)
    load, z_send, z_recv, a_send, a_recv, b_send, b_recv, index_load, told = scratch
    ep, dp = lax.axis_index("ep"), lax.axis_index("dp")
    _, blocks, depth, cols = out_ref.shape
    rows = blocks * depth
    total = offsets_ref.shape[1]
    index_copies = [
        pltpu.make_async_copy(src, dst, index_load.at[i])
        for i, (src, dst) in enumerate(zip(indices_in, (ids_ref, offsets_ref, writers_ref), strict=True))
    ]
    pair = rows // n_dp
    aligned = depth % PACK == 0
    m_ep, m_dp = blocks // n_ep, blocks // n_dp
    z_order = sorted(range(1, n_dp))
    e_order = sorted(range(1, n_ep), key=lambda o: (o == 1, o % 2, -o))

    def span(c):
        f = c % FIELDS
        return pl.ds(0, split[f]) if c < FIELDS else pl.ds(split[f], cols - split[f])

    def load_copy(c):
        return pltpu.make_async_copy(fields_in[c % FIELDS].at[:, span(c)], wide[c], load.at[c])


    for copy in index_copies:
        copy.start()
    load_copy(5).start()
    load_copy(0).start()

    barrier = pltpu.get_barrier_semaphore()
    even = ep % 2 == 0
    odd_of_pair = ep + 1 - ep % 2
    for o in range(1, n_dp):
        pl.semaphore_signal(
            barrier, inc=1, device_id={"dp": partner(dp, o, n_dp), "ep": odd_of_pair}, device_id_type=MESH
        )
    for o in range(1, n_ep):
        @pl.when(partner(ep, o, n_ep) % 2 == 0)
        def _(o=o):
            pl.semaphore_signal(barrier, inc=1, device_id={"ep": partner(ep, o, n_ep)}, device_id_type=MESH)

    for c in (3, 1, 4, 2):
        load_copy(c).start()

    def tell_partner():
        pl.semaphore_signal(told, inc=1, device_id={"ep": partner(ep, 1, n_ep)}, device_id_type=MESH)

    def ep_group_is_in():
        @pl.when(even)
        def _():
            pl.semaphore_wait(barrier, n_ep - 1)
            tell_partner()

        @pl.when(jnp.logical_not(even))
        def _():
            pl.semaphore_wait(told, 1)

    def dp_group_is_in():
        @pl.when(jnp.logical_not(even))
        def _():
            pl.semaphore_wait(barrier, 2 * (n_dp - 1))
            tell_partner()

        @pl.when(even)
        def _():
            pl.semaphore_wait(told, 1)

    def remote(src, dst, send, recv, axis, peer):
        return pltpu.make_async_remote_copy(
            src_ref=src, dst_ref=dst, send_sem=send, recv_sem=recv,
            device_id={axis: peer}, device_id_type=MESH,
        )

    def z_refs(c):
        return (ready[c], mid[c]) if c < FIELDS else (early[c - FIELDS], late[c - FIELDS])

    def a_ref(c):
        return placed[c] if c < FIELDS else ready[c]

    def b_ref(c):
        return out_ref.at[c, :, :, span(c)] if c < FIELDS else mid[c]

    def z_copies(c):
        src, dst = z_refs(c)
        return [
            remote(
                src.at[pl.ds(partner(dp, o, n_dp) * m_dp, m_dp)], dst.at[pl.ds(dp * m_dp, m_dp)],
                z_send.at[c], z_recv.at[c], "dp", partner(dp, o, n_dp),
            )
            for o in z_order
        ]

    def a_copies(c):
        return [
            remote(
                a_ref(c).at[pl.ds(partner(ep, o, n_ep) * m_ep, m_ep)], e1[c].at[ep],
                a_send.at[c], a_recv.at[c], "ep", partner(ep, o, n_ep),
            )
            for o in e_order
        ]

    def b_copies(c):
        return [
            remote(
                sel[c].at[partner(ep, o, n_ep)], b_ref(c).at[pl.ds(ep * m_ep, m_ep)],
                b_send.at[c], b_recv.at[c], "ep", partner(ep, o, n_ep),
            )
            for o in e_order
        ]

    def z_all(c):
        src, dst = z_refs(c)
        part = pl.ds(0, (n_dp - 1) * m_dp)
        return remote(src.at[part], dst.at[part], z_send.at[c], z_recv.at[c], "dp", partner(dp, 1, n_dp))

    def a_all(c):
        part = pl.ds(0, (n_ep - 1) * m_ep)
        return remote(
            a_ref(c).at[part], e1[c].at[pl.ds(0, n_ep - 1)], a_send.at[c], a_recv.at[c], "ep", partner(ep, 1, n_ep)
        )

    def b_all(c):
        part = pl.ds(0, (n_ep - 1) * m_ep)
        return remote(
            sel[c].at[pl.ds(0, n_ep - 1)], b_ref(c).at[part], b_send.at[c], b_recv.at[c], "ep", partner(ep, 1, n_ep)
        )

    def start(copies):
        for copy in copies:
            copy.start()

    def make_order():
        def rank_of(e):
            rank = jnp.int32(0)
            for f in range(n_ep):
                tied = (ids_ref[f] == ids_ref[e]) & (f < e)
                rank = rank + ((ids_ref[f] < ids_ref[e]) | tied).astype(I32)
            return rank

        @pl.loop(0, n_ep)
        def _(e):
            rank_ref[e] = rank_of(e)

        @pl.loop(0, n_ep)
        def _(k):
            source = jnp.int32(0)
            for e in range(n_ep):
                source = source + jnp.where(rank_ref[e] == k, e, 0)
            order_ref[k] = source

    def groups_of(writer):
        return (writer == iota((PACK, writer.shape[1]), 0).astype(writer.dtype)).astype(F32)

    def rank_in(groups):
        return dot(groups.astype(BF16), ahead[...])

    def pick(table, s):
        offsets = offsets_ref[:, pl.ds(pl.multiple_of(s * rows, rows), rows)]
        return dot(table, as_bf16(offsets == iota((total, rows), 0)))

    def writer_and_rank(writer):
        groups = groups_of(writer)
        return jnp.sum(groups * rank_in(groups), axis=0, keepdims=True)

    def make_position():
        ahead[...] = as_bf16(iota((rows, rows), 0) < iota((rows, rows), 1))
        picked = pick(stack_rows([writers_ref[...].astype(F32)], total), dp)
        writer = row_of(picked, 0)
        position_ref[...] = (writer * pair + writer_and_rank(writer)).astype(I32)

    def make_targets():
        carry = jnp.zeros((PACK, 1), F32)
        within = []
        for s in range(n_dp):
            groups = groups_of(writers_ref[:, s * rows : (s + 1) * rows])
            count = rank_in(groups) + carry
            carry = carry + jnp.sum(groups, axis=1, keepdims=True)
            within.append(jnp.sum(groups * count, axis=0, keepdims=True).astype(I32))
        place = jnp.concatenate(within, axis=1)
        table = stack_rows(
            [writers_ref[...].astype(F32), (place // 256).astype(F32), (place % 256).astype(F32)], total
        )

        @pl.loop(0, n_dp)
        def _(s):
            picked = pick(table, s)
            writer = row_of(picked, 0)
            here = pl.ds(pl.multiple_of(s * rows, rows), rows)
            target_ref[:, here] = (writer * rows + row_of(picked, 1) * 256 + row_of(picked, 2)).astype(I32)
            arrives_ref[:, here] = (writer_and_rank(writer)).astype(I32) + s * pair

    def after_of(i, j, size):
        return lax.dot_general(
            one_hot(target_ref, dp * rows + i * size, size), one_hot(arrives_ref, j * size, size),
            (((1,), (1,)), ((), ())), preferred_element_type=F32,
        ).astype(BF16)

    def permute(matrix, src, dst):
        def body(part):
            if aligned:
                x = src[:, :, part].reshape(rows, part.size)
                dst[:, :, part] = dot(matrix[...], x).astype(BF16).reshape(blocks, depth, part.size)
            else:
                @pl.loop(0, blocks)
                def _(i):
                    def add(j, so_far):
                        return so_far + dot(matrix[i, j], src[j, :, part])

                    dst[i, :, part] = lax.fori_loop(
                        0, blocks, add, jnp.zeros((depth, part.size), F32)
                    ).astype(BF16)

        column_tiles(dst.shape[2], body)

    def sort(c):
        load_copy(c).wait()

        def body(part):
            x = wide[c][:, part].astype(BF16)
            if aligned:
                ready[c][:, :, part] = dot(before[...], x).astype(BF16).reshape(blocks, depth, part.size)
            else:
                @pl.loop(0, blocks)
                def _(i):
                    ready[c][i, :, part] = dot(one_hot(position_ref, i * depth, depth), x).astype(BF16)

        column_tiles(ready[c].shape[2], body)

    def narrow(c):
        load_copy(c).wait()

        def body(part):
            x = wide[c][:, part].astype(BF16)
            if aligned:
                ready[c][:, :, part] = x.reshape(blocks, depth, part.size)
            else:
                @pl.loop(0, blocks)
                def _(i):
                    keep = as_bf16(iota((depth, rows), 0) + i * depth == iota((depth, rows), 1))
                    ready[c][i, :, part] = dot(keep, x).astype(BF16)

        column_tiles(ready[c].shape[2], body)

    def z_start(c):
        start(z_copies(c))
        src, dst = z_refs(c)
        own = pl.ds(dp * m_dp, m_dp)
        dst[own] = src[own]

    def a_start(c):
        start(a_copies(c))
        e1[c][ep] = a_ref(c)[pl.ds(ep * m_ep, m_ep)]

    def a_to_b(c):
        a_all(c).wait_recv()
        for k in range(n_ep):
            sel[c][k] = e1[c][order_ref[k]]
        start(b_copies(c))
        b_ref(c)[pl.ds(ep * m_ep, m_ep)] = sel[c][ep]

    def z_to_a(c):
        z_all(c).wait_recv()
        permute(after, mid[c], placed[c])
        a_start(c)

    def back(c):
        b_all(c).wait_recv()
        permute(before, mid[c], early[c - FIELDS])

    def b_to_z(c):
        back(c)
        z_start(c)

    def z_to_a_and_z(c, following):
        z_all(c).wait_recv()
        z_start(following)
        permute(after, mid[c], placed[c])
        a_start(c)

    def finish(c):
        z_all(c).wait_recv()
        permute(after, late[c - FIELDS], out_ref.at[c - FIELDS, :, :, span(c)])

    narrow(5)
    ep_group_is_in()
    a_start(5)
    for copy in index_copies:
        copy.wait()
    make_position()
    if aligned:
        before[...] = one_hot(position_ref, 0, rows)
    sort(0)
    dp_group_is_in()
    z_start(0)
    narrow(3)
    a_start(3)
    sort(1)
    z_start(1)
    narrow(4)
    a_start(4)
    sort(2)
    z_start(2)
    make_order()
    make_targets()
    if aligned:
        after[...] = after_of(0, 0, rows)
    else:
        @pl.loop(0, blocks)
        def _(i):
            @pl.loop(0, blocks)
            def _(j):
                after[i, j] = after_of(i, j, depth)
                mine = as_bf16(position_ref[...] == iota((depth, rows), 0) + i * depth)
                whose = as_bf16(iota((depth, rows), 1) == iota((depth, rows), 0) + j * depth)
                before[i, j] = lax.dot_general(
                    mine, whose, (((1,), (1,)), ((), ())), preferred_element_type=F32
                ).astype(BF16)
    a_to_b(3)
    z_to_a(0)
    a_to_b(4)
    a_to_b(5)
    z_to_a(1)
    a_to_b(0)
    back(3)
    z_to_a_and_z(2, 3)
    b_to_z(4)
    b_to_z(5)
    a_to_b(1)
    finish(3)
    a_to_b(2)
    finish(4)
    b_all(0).wait_recv()
    b_all(1).wait_recv()
    finish(5)
    b_all(2).wait_recv()
    for c in range(chunks):
        z_all(c).wait_send()
        a_all(c).wait_send()
        b_all(c).wait_send()


def exchange(expert_ids, offsets, writers, arrays, n_ep, n_dp):
    rows, cols = arrays[0].shape
    total = offsets.shape[1]
    depth = math.gcd(rows // n_dp, rows // n_ep)
    blocks = rows // depth
    split = widths(cols)
    per = blocks // n_ep
    size = split + [cols - w for w in split]
    dma = pltpu.SemaphoreType.DMA
    vmem = pl.BlockSpec(memory_space=pltpu.VMEM)
    square = (rows, rows) if depth % PACK == 0 else (blocks, blocks, depth, depth)

    def each(shape, widths_of, kind=BF16):
        return [pltpu.VMEM((*shape, w), kind) for w in widths_of]

    first, last = size[:FIELDS], size[FIELDS:]
    chunks = 2 * FIELDS
    return pl.pallas_call(
        functools.partial(exchange_kernel, n_ep, n_dp, split),
        out_shape=pltpu.VMEM((FIELDS, blocks, depth, cols), BF16),
        in_specs=[pl.BlockSpec(memory_space=pl.ANY)] * (3 + FIELDS),
        out_specs=vmem,
        scratch_shapes=each((rows,), size, F32)
        + each((blocks, depth), size)
        + each((blocks, depth), size)
        + each((n_ep, per, depth), size)
        + each((n_ep, per, depth), size)
        + each((blocks, depth), first)
        + each((blocks, depth), last)
        + each((blocks, depth), last)
        + [
            pltpu.SMEM((n_ep,), I32),
            pltpu.VMEM((1, total), I32),
            pltpu.VMEM((1, total), I32),
            pltpu.SMEM((n_ep,), I32),
            pltpu.SMEM((n_ep,), I32),
            pltpu.VMEM((1, rows), I32),
            pltpu.VMEM((1, total), I32),
            pltpu.VMEM((1, total), I32),
            pltpu.VMEM(square, BF16),
            pltpu.VMEM(square, BF16),
            pltpu.VMEM((rows, rows), BF16),
            dma((chunks,)),
            dma((chunks,)),
            dma((chunks,)),
            dma((chunks,)),
            dma((chunks,)),
            dma((chunks,)),
            dma((chunks,)),
            dma((3,)),
            pltpu.SemaphoreType.REGULAR,
        ],
        compiler_params=pltpu.CompilerParams(
            collective_id=0, has_side_effects=True, vmem_limit_bytes=54 * 2**20
        ),
    )(expert_ids, offsets, writers, *arrays)


def on_device(master_weights, first_moment, second_moment, expert_ids, bucket_offsets, writer_rank):
    n_dp, n_ep = lax.axis_size("dp"), lax.axis_size("ep")
    _, rows, cols = master_weights.shape
    total = bucket_offsets.shape[0]
    arrays = (master_weights[0], first_moment[0], second_moment[0])
    saved = exchange(
        expert_ids, bucket_offsets.reshape(1, total), writer_rank.reshape(1, total), arrays, n_ep, n_dp
    )
    return saved.reshape(FIELDS, 1, rows, cols)


def solution(mesh):
    return jax.shard_map(
        on_device,
        mesh=mesh,
        in_specs=(P("ep", "dp", None), P("ep", "dp", None), P("ep", "dp", None), P(), P(), P()),
        out_specs=P(None, "ep", "dp", None),
        check_vma=False,
    )
```

```python
import functools
import math

import jax
import jax.numpy as jnp
from jax import lax
from jax.experimental import pallas as pl
from jax.experimental.pallas import tpu as pltpu
from jax.sharding import PartitionSpec as P

MESH = pl.DeviceIdType.MESH
FIELDS = 3
PACK = 16
BF16, F32, I32 = jnp.bfloat16, jnp.float32, jnp.int32


def cut(total, parts):
    units = total // 128
    return 128 * min(max(round(units * parts), 1), units - 1)


def widths(cols):
    if cols % 128:
        return [cols // 2] * FIELDS
    return [cut(cols, 2 / 7), cut(cols, 1 / 2), cut(cols, 5 / 7)]


def as_bf16(mask):
    return mask.astype(F32).astype(BF16)


def dot(left, right):
    return jnp.dot(left, right, preferred_element_type=F32)


def iota(shape, axis):
    return lax.broadcasted_iota(I32, shape, axis)


def one_hot(index_ref, first, depth):
    return as_bf16(index_ref[...] == iota((depth, index_ref.shape[1]), 0) + first)


def row_of(stack, row):
    return jnp.sum(jnp.where(iota(stack.shape, 0) == row, stack, 0.0), axis=0, keepdims=True)


def stack_rows(rows, width):
    out = jnp.zeros((PACK, width), F32)
    for i, row in enumerate(rows):
        out = jnp.where(iota((PACK, width), 0) == i, row, out)
    return out.astype(BF16)


def column_tiles(cols, body):
    tile = next((t for t in (512, 256, 128) if cols % t == 0), cols)

    @pl.loop(0, cols // tile)
    def _(i):
        body(pl.ds(pl.multiple_of(i * tile, tile), tile))


def partner(me, offset, n):
    out, bit = 0, 1
    while bit < n:
        out = out + ((me // bit + (offset // bit) % 2) % 2) * bit
        bit *= 2
    return out


def permute_rows(aligned, matrix, src, dst):
    blocks, depth, width = dst.shape
    rows = blocks * depth

    def body(part):
        if aligned:
            x = src[:, :, part].reshape(rows, part.size)
            dst[:, :, part] = dot(matrix[...], x).astype(BF16).reshape(blocks, depth, part.size)
        else:
            @pl.loop(0, blocks)
            def _(i):
                def add(j, so_far):
                    return so_far + dot(matrix[i, j], src[j, :, part])

                dst[i, :, part] = lax.fori_loop(
                    0, blocks, add, jnp.zeros((depth, part.size), F32)
                ).astype(BF16)

    column_tiles(width, body)


def last_kernel(split, most_ref, late_ref, after_ref, out_ref, placed, store):
    blocks, depth, cols = most_ref.shape[1:]
    parts = 4 if blocks % 4 == 0 else 1
    some = blocks // parts
    f = FIELDS - 1

    def copies(field, width):
        return [
            pltpu.make_async_copy(
                most_ref.at[field, pl.ds(i * some, some), :, pl.ds(0, width)],
                out_ref.at[field, pl.ds(i * some, some), :, pl.ds(0, width)],
                store.at[field, i],
            )
            for i in range(parts)
        ]

    moves = [copy for field in range(FIELDS) for copy in copies(field, cols if field < f else split[f])]
    for copy in moves:
        copy.start()
    permute_rows(depth % PACK == 0, after_ref, late_ref, placed)
    rest = pltpu.make_async_copy(placed, out_ref.at[f, :, :, pl.ds(split[f], cols - split[f])], store.at[FIELDS, 0])
    rest.start()
    for copy in moves:
        copy.wait()
    rest.wait()


def exchange_kernel(n_ep, n_dp, split, *refs_in):
    indices_in = refs_in[:3]
    fields_in, out_ref, scratch = refs_in[3 : 3 + FIELDS], refs_in[3 + FIELDS], list(refs_in[6 + FIELDS :])
    last_late, after = refs_in[4 + FIELDS : 6 + FIELDS]

    def take(count):
        head = scratch[:count]
        del scratch[:count]
        return head

    chunks = 2 * FIELDS
    wide, ready, mid, e1, sel = (take(chunks) for _ in range(5))
    placed, early, late = take(FIELDS), take(FIELDS), take(FIELDS - 1) + [last_late]
    ids_ref, offsets_ref, writers_ref = take(3)
    rank_ref, order_ref, position_ref, target_ref, arrives_ref, before, ahead = take(7)
    load, z_send, z_recv, a_send, a_recv, b_send, b_recv, index_load = scratch
    ep, dp = lax.axis_index("ep"), lax.axis_index("dp")
    _, blocks, depth, cols = out_ref.shape
    rows = blocks * depth
    total = offsets_ref.shape[1]
    index_copies = [
        pltpu.make_async_copy(src, dst, index_load.at[i])
        for i, (src, dst) in enumerate(zip(indices_in, (ids_ref, offsets_ref, writers_ref), strict=True))
    ]
    pair = rows // n_dp
    aligned = depth % PACK == 0
    m_ep, m_dp = blocks // n_ep, blocks // n_dp
    z_order = sorted(range(1, n_dp))
    e_order = sorted(range(1, n_ep), key=lambda o: (o == 1, o % 2, -o))

    def span(c):
        f = c % FIELDS
        return pl.ds(0, split[f]) if c < FIELDS else pl.ds(split[f], cols - split[f])

    def load_copy(c):
        return pltpu.make_async_copy(fields_in[c % FIELDS].at[:, span(c)], wide[c], load.at[c])


    for copy in index_copies:
        copy.start()
    load_copy(5).start()
    load_copy(0).start()

    barrier = pltpu.get_barrier_semaphore()
    for o in range(1, n_dp):
        pl.semaphore_signal(barrier, inc=1, device_id={"dp": partner(dp, o, n_dp)}, device_id_type=MESH)
    for o in range(1, n_ep):
        pl.semaphore_signal(barrier, inc=1, device_id={"ep": partner(ep, o, n_ep)}, device_id_type=MESH)

    for c in (3, 1, 4, 2):
        load_copy(c).start()

    def remote(src, dst, send, recv, axis, peer):
        return pltpu.make_async_remote_copy(
            src_ref=src, dst_ref=dst, send_sem=send, recv_sem=recv,
            device_id={axis: peer}, device_id_type=MESH,
        )

    def z_refs(c):
        return (ready[c], mid[c]) if c < FIELDS else (early[c - FIELDS], late[c - FIELDS])

    def a_ref(c):
        return placed[c] if c < FIELDS else ready[c]

    def b_ref(c):
        return out_ref.at[c, :, :, span(c)] if c < FIELDS else mid[c]

    def z_copies(c):
        src, dst = z_refs(c)
        return [
            remote(
                src.at[pl.ds(partner(dp, o, n_dp) * m_dp, m_dp)], dst.at[pl.ds(dp * m_dp, m_dp)],
                z_send.at[c], z_recv.at[c], "dp", partner(dp, o, n_dp),
            )
            for o in z_order
        ]

    def a_copies(c):
        return [
            remote(
                a_ref(c).at[pl.ds(partner(ep, o, n_ep) * m_ep, m_ep)], e1[c].at[ep],
                a_send.at[c], a_recv.at[c], "ep", partner(ep, o, n_ep),
            )
            for o in e_order
        ]

    def b_copies(c):
        return [
            remote(
                sel[c].at[partner(ep, o, n_ep)], b_ref(c).at[pl.ds(ep * m_ep, m_ep)],
                b_send.at[c], b_recv.at[c], "ep", partner(ep, o, n_ep),
            )
            for o in e_order
        ]

    def z_all(c):
        src, dst = z_refs(c)
        part = pl.ds(0, (n_dp - 1) * m_dp)
        return remote(src.at[part], dst.at[part], z_send.at[c], z_recv.at[c], "dp", partner(dp, 1, n_dp))

    def a_all(c):
        part = pl.ds(0, (n_ep - 1) * m_ep)
        return remote(
            a_ref(c).at[part], e1[c].at[pl.ds(0, n_ep - 1)], a_send.at[c], a_recv.at[c], "ep", partner(ep, 1, n_ep)
        )

    def b_all(c):
        part = pl.ds(0, (n_ep - 1) * m_ep)
        return remote(
            sel[c].at[pl.ds(0, n_ep - 1)], b_ref(c).at[part], b_send.at[c], b_recv.at[c], "ep", partner(ep, 1, n_ep)
        )

    def start(copies):
        for copy in copies:
            copy.start()

    def make_order():
        def rank_of(e):
            rank = jnp.int32(0)
            for f in range(n_ep):
                tied = (ids_ref[f] == ids_ref[e]) & (f < e)
                rank = rank + ((ids_ref[f] < ids_ref[e]) | tied).astype(I32)
            return rank

        @pl.loop(0, n_ep)
        def _(e):
            rank_ref[e] = rank_of(e)

        @pl.loop(0, n_ep)
        def _(k):
            source = jnp.int32(0)
            for e in range(n_ep):
                source = source + jnp.where(rank_ref[e] == k, e, 0)
            order_ref[k] = source

    def groups_of(writer):
        return (writer == iota((PACK, writer.shape[1]), 0).astype(writer.dtype)).astype(F32)

    def rank_in(groups):
        return dot(groups.astype(BF16), ahead[...])

    def pick(table, s):
        offsets = offsets_ref[:, pl.ds(pl.multiple_of(s * rows, rows), rows)]
        return dot(table, as_bf16(offsets == iota((total, rows), 0)))

    def writer_and_rank(writer):
        groups = groups_of(writer)
        return jnp.sum(groups * rank_in(groups), axis=0, keepdims=True)

    def make_position():
        ahead[...] = as_bf16(iota((rows, rows), 0) < iota((rows, rows), 1))
        picked = pick(stack_rows([writers_ref[...].astype(F32)], total), dp)
        writer = row_of(picked, 0)
        position_ref[...] = (writer * pair + writer_and_rank(writer)).astype(I32)

    def make_targets():
        carry = jnp.zeros((PACK, 1), F32)
        within = []
        for s in range(n_dp):
            groups = groups_of(writers_ref[:, s * rows : (s + 1) * rows])
            count = rank_in(groups) + carry
            carry = carry + jnp.sum(groups, axis=1, keepdims=True)
            within.append(jnp.sum(groups * count, axis=0, keepdims=True).astype(I32))
        place = jnp.concatenate(within, axis=1)
        table = stack_rows(
            [writers_ref[...].astype(F32), (place // 256).astype(F32), (place % 256).astype(F32)], total
        )

        @pl.loop(0, n_dp)
        def _(s):
            picked = pick(table, s)
            writer = row_of(picked, 0)
            here = pl.ds(pl.multiple_of(s * rows, rows), rows)
            target_ref[:, here] = (writer * rows + row_of(picked, 1) * 256 + row_of(picked, 2)).astype(I32)
            arrives_ref[:, here] = (writer_and_rank(writer)).astype(I32) + s * pair

    def after_of(i, j, size):
        return lax.dot_general(
            one_hot(target_ref, dp * rows + i * size, size), one_hot(arrives_ref, j * size, size),
            (((1,), (1,)), ((), ())), preferred_element_type=F32,
        ).astype(BF16)

    permute = functools.partial(permute_rows, aligned)

    def sort(c):
        load_copy(c).wait()

        def body(part):
            x = wide[c][:, part].astype(BF16)
            if aligned:
                ready[c][:, :, part] = dot(before[...], x).astype(BF16).reshape(blocks, depth, part.size)
            else:
                @pl.loop(0, blocks)
                def _(i):
                    ready[c][i, :, part] = dot(one_hot(position_ref, i * depth, depth), x).astype(BF16)

        column_tiles(ready[c].shape[2], body)

    def narrow(c):
        load_copy(c).wait()

        def body(part):
            x = wide[c][:, part].astype(BF16)
            if aligned:
                ready[c][:, :, part] = x.reshape(blocks, depth, part.size)
            else:
                @pl.loop(0, blocks)
                def _(i):
                    keep = as_bf16(iota((depth, rows), 0) + i * depth == iota((depth, rows), 1))
                    ready[c][i, :, part] = dot(keep, x).astype(BF16)

        column_tiles(ready[c].shape[2], body)

    def z_start(c):
        start(z_copies(c))
        src, dst = z_refs(c)
        own = pl.ds(dp * m_dp, m_dp)
        dst[own] = src[own]

    def a_start(c):
        start(a_copies(c))
        e1[c][ep] = a_ref(c)[pl.ds(ep * m_ep, m_ep)]

    def a_to_b(c):
        a_all(c).wait_recv()
        for k in range(n_ep):
            sel[c][k] = e1[c][order_ref[k]]
        start(b_copies(c))
        b_ref(c)[pl.ds(ep * m_ep, m_ep)] = sel[c][ep]

    def z_to_a(c):
        z_all(c).wait_recv()
        permute(after, mid[c], placed[c])
        a_start(c)

    def b_to_z(c):
        b_all(c).wait_recv()
        permute(before, mid[c], early[c - FIELDS])
        z_start(c)

    def finish(c):
        z_all(c).wait_recv()
        permute(after, late[c - FIELDS], out_ref.at[c - FIELDS, :, :, span(c)])

    narrow(5)
    for copy in index_copies:
        copy.wait()
    make_position()
    if aligned:
        before[...] = one_hot(position_ref, 0, rows)
    sort(0)
    pl.semaphore_wait(barrier, n_dp + n_ep - 2)
    a_start(5)
    z_start(0)
    narrow(3)
    a_start(3)
    sort(1)
    z_start(1)
    narrow(4)
    a_start(4)
    sort(2)
    z_start(2)
    make_order()
    make_targets()
    if aligned:
        after[...] = after_of(0, 0, rows)
    else:
        @pl.loop(0, blocks)
        def _(i):
            @pl.loop(0, blocks)
            def _(j):
                after[i, j] = after_of(i, j, depth)
                mine = as_bf16(position_ref[...] == iota((depth, rows), 0) + i * depth)
                whose = as_bf16(iota((depth, rows), 1) == iota((depth, rows), 0) + j * depth)
                before[i, j] = lax.dot_general(
                    mine, whose, (((1,), (1,)), ((), ())), preferred_element_type=F32
                ).astype(BF16)
    a_to_b(3)
    z_to_a(0)
    a_to_b(4)
    a_to_b(5)
    z_to_a(1)
    a_to_b(0)
    b_to_z(3)
    z_to_a(2)
    b_to_z(4)
    b_to_z(5)
    a_to_b(1)
    a_to_b(2)
    finish(3)
    finish(4)
    b_all(0).wait_recv()
    b_all(1).wait_recv()
    z_all(5).wait_recv()
    b_all(2).wait_recv()
    for c in range(chunks):
        z_all(c).wait_send()
        a_all(c).wait_send()
        b_all(c).wait_send()


def exchange(expert_ids, offsets, writers, arrays, n_ep, n_dp):
    rows, cols = arrays[0].shape
    total = offsets.shape[1]
    depth = math.gcd(rows // n_dp, rows // n_ep)
    blocks = rows // depth
    split = widths(cols)
    per = blocks // n_ep
    size = split + [cols - w for w in split]
    dma = pltpu.SemaphoreType.DMA
    vmem = pl.BlockSpec(memory_space=pltpu.VMEM)
    square = (rows, rows) if depth % PACK == 0 else (blocks, blocks, depth, depth)

    def each(shape, widths_of, kind=BF16):
        return [pltpu.VMEM((*shape, w), kind) for w in widths_of]

    first, last = size[:FIELDS], size[FIELDS:]
    chunks = 2 * FIELDS
    most, late, after = pl.pallas_call(
        functools.partial(exchange_kernel, n_ep, n_dp, split),
        out_shape=[
            pltpu.VMEM((FIELDS, blocks, depth, cols), BF16),
            pltpu.VMEM((blocks, depth, last[-1]), BF16),
            pltpu.VMEM(square, BF16),
        ],
        in_specs=[pl.BlockSpec(memory_space=pl.ANY)] * (3 + FIELDS),
        out_specs=[vmem] * 3,
        scratch_shapes=each((rows,), size, F32)
        + each((blocks, depth), size)
        + each((blocks, depth), size)
        + each((n_ep, per, depth), size)
        + each((n_ep, per, depth), size)
        + each((blocks, depth), first)
        + each((blocks, depth), last)
        + each((blocks, depth), last[:-1])
        + [
            pltpu.SMEM((n_ep,), I32),
            pltpu.VMEM((1, total), I32),
            pltpu.VMEM((1, total), I32),
            pltpu.SMEM((n_ep,), I32),
            pltpu.SMEM((n_ep,), I32),
            pltpu.VMEM((1, rows), I32),
            pltpu.VMEM((1, total), I32),
            pltpu.VMEM((1, total), I32),
            pltpu.VMEM(square, BF16),
            pltpu.VMEM((rows, rows), BF16),
            dma((chunks,)),
            dma((chunks,)),
            dma((chunks,)),
            dma((chunks,)),
            dma((chunks,)),
            dma((chunks,)),
            dma((chunks,)),
            dma((3,)),
        ],
        compiler_params=pltpu.CompilerParams(
            collective_id=0, has_side_effects=True, vmem_limit_bytes=54 * 2**20
        ),
    )(expert_ids, offsets, writers, *arrays)
    in_vmem = [pltpu.with_memory_space_constraint(x, pltpu.VMEM) for x in (most, late, after)]
    return pl.pallas_call(
        functools.partial(last_kernel, split),
        out_shape=jax.ShapeDtypeStruct((FIELDS, blocks, depth, cols), BF16),
        in_specs=[vmem] * 3,
        out_specs=pl.BlockSpec(memory_space=pl.ANY),
        scratch_shapes=[pltpu.VMEM((blocks, depth, last[-1]), BF16), dma((FIELDS + 1, 4))],
        compiler_params=pltpu.CompilerParams(vmem_limit_bytes=8 * 2**20),
    )(*in_vmem)


def on_device(master_weights, first_moment, second_moment, expert_ids, bucket_offsets, writer_rank):
    n_dp, n_ep = lax.axis_size("dp"), lax.axis_size("ep")
    _, rows, cols = master_weights.shape
    total = bucket_offsets.shape[0]
    arrays = (master_weights[0], first_moment[0], second_moment[0])
    saved = exchange(
        expert_ids, bucket_offsets.reshape(1, total), writer_rank.reshape(1, total), arrays, n_ep, n_dp
    )
    return saved.reshape(FIELDS, 1, rows, cols)


def solution(mesh):
    return jax.shard_map(
        on_device,
        mesh=mesh,
        in_specs=(P("ep", "dp", None), P("ep", "dp", None), P("ep", "dp", None), P(), P(), P()),
        out_specs=P(None, "ep", "dp", None),
        check_vma=False,
    )
```

```python
import functools
import math

import jax
import jax.numpy as jnp
from jax import lax
from jax.experimental import pallas as pl
from jax.experimental.pallas import tpu as pltpu
from jax.sharding import PartitionSpec as P

MESH = pl.DeviceIdType.MESH
FIELDS = 3
PACK = 16
BF16, F32, I32 = jnp.bfloat16, jnp.float32, jnp.int32


def cut(total, parts):
    units = total // 128
    return 128 * min(max(round(units * parts), 1), units - 1)


def widths(cols):
    if cols % 128:
        return [cols // 2] * FIELDS
    return [cut(cols, 2 / 7), cut(cols, 1 / 2), cut(cols, 5 / 7)]


def as_bf16(mask):
    return mask.astype(F32).astype(BF16)


def dot(left, right):
    return jnp.dot(left, right, preferred_element_type=F32)


def iota(shape, axis):
    return lax.broadcasted_iota(I32, shape, axis)


def one_hot(index_ref, first, depth):
    return as_bf16(index_ref[...] == iota((depth, index_ref.shape[1]), 0) + first)


def row_of(stack, row):
    return jnp.sum(jnp.where(iota(stack.shape, 0) == row, stack, 0.0), axis=0, keepdims=True)


def stack_rows(rows, width):
    out = jnp.zeros((PACK, width), F32)
    for i, row in enumerate(rows):
        out = jnp.where(iota((PACK, width), 0) == i, row, out)
    return out.astype(BF16)


def column_tiles(cols, body):
    tile = next((t for t in (512, 256, 128) if cols % t == 0), cols)

    @pl.loop(0, cols // tile)
    def _(i):
        body(pl.ds(pl.multiple_of(i * tile, tile), tile))


def partner(me, offset, n):
    out, bit = 0, 1
    while bit < n:
        out = out + ((me // bit + (offset // bit) % 2) % 2) * bit
        bit *= 2
    return out


def permute_rows(aligned, matrix, src, dst):
    blocks, depth, width = dst.shape
    rows = blocks * depth

    def body(part):
        if aligned:
            x = src[:, :, part].reshape(rows, part.size)
            dst[:, :, part] = dot(matrix[...], x).astype(BF16).reshape(blocks, depth, part.size)
        else:
            @pl.loop(0, blocks)
            def _(i):
                def add(j, so_far):
                    return so_far + dot(matrix[i, j], src[j, :, part])

                dst[i, :, part] = lax.fori_loop(
                    0, blocks, add, jnp.zeros((depth, part.size), F32)
                ).astype(BF16)

    column_tiles(width, body)


def last_kernel(split, most_ref, late_ref, after_ref, out_ref, placed, store):
    blocks, depth, cols = most_ref.shape[1:]
    parts = 1
    some = blocks // parts
    f = FIELDS - 1

    def copies(field, width):
        return [
            pltpu.make_async_copy(
                most_ref.at[field, pl.ds(i * some, some), :, pl.ds(0, width)],
                out_ref.at[field, pl.ds(i * some, some), :, pl.ds(0, width)],
                store.at[field, i],
            )
            for i in range(parts)
        ]

    moves = [copy for field in range(FIELDS) for copy in copies(field, cols if field < f else split[f])]
    for copy in moves:
        copy.start()
    permute_rows(depth % PACK == 0, after_ref, late_ref, placed)
    rest = pltpu.make_async_copy(placed, out_ref.at[f, :, :, pl.ds(split[f], cols - split[f])], store.at[FIELDS, 0])
    rest.start()
    for copy in moves:
        copy.wait()
    rest.wait()


def exchange_kernel(n_ep, n_dp, split, *refs_in):
    indices_in = refs_in[:3]
    fields_in, out_ref, scratch = refs_in[3 : 3 + FIELDS], refs_in[3 + FIELDS], list(refs_in[6 + FIELDS :])
    last_late, after = refs_in[4 + FIELDS : 6 + FIELDS]

    def take(count):
        head = scratch[:count]
        del scratch[:count]
        return head

    chunks = 2 * FIELDS
    wide, ready, mid, e1, sel = (take(chunks) for _ in range(5))
    placed, early, late = take(FIELDS), take(FIELDS), take(FIELDS - 1) + [last_late]
    ids_ref, offsets_ref, writers_ref = take(3)
    rank_ref, order_ref, position_ref, target_ref, arrives_ref, before, ahead = take(7)
    load, leave, z_recv, a_recv, b_recv, index_load = scratch
    ep, dp = lax.axis_index("ep"), lax.axis_index("dp")
    _, blocks, depth, cols = out_ref.shape
    rows = blocks * depth
    total = offsets_ref.shape[1]
    index_copies = [
        pltpu.make_async_copy(src, dst, index_load.at[i])
        for i, (src, dst) in enumerate(zip(indices_in, (ids_ref, offsets_ref, writers_ref), strict=True))
    ]
    pair = rows // n_dp
    aligned = depth % PACK == 0
    m_ep, m_dp = blocks // n_ep, blocks // n_dp
    z_order = sorted(range(1, n_dp))
    e_order = sorted(range(1, n_ep), key=lambda o: (o == 1, o % 2, -o))

    def span(c):
        f = c % FIELDS
        return pl.ds(0, split[f]) if c < FIELDS else pl.ds(split[f], cols - split[f])

    def load_copy(c):
        return pltpu.make_async_copy(fields_in[c % FIELDS].at[:, span(c)], wide[c], load.at[c])


    for copy in index_copies:
        copy.start()
    load_copy(5).start()
    load_copy(0).start()

    barrier = pltpu.get_barrier_semaphore()
    for o in range(1, n_dp):
        pl.semaphore_signal(barrier, inc=1, device_id={"dp": partner(dp, o, n_dp)}, device_id_type=MESH)
    for o in range(1, n_ep):
        pl.semaphore_signal(barrier, inc=1, device_id={"ep": partner(ep, o, n_ep)}, device_id_type=MESH)

    for c in (3, 1, 4, 2):
        load_copy(c).start()

    def remote(src, dst, send, recv, axis, peer):
        return pltpu.make_async_remote_copy(
            src_ref=src, dst_ref=dst, send_sem=send, recv_sem=recv,
            device_id={axis: peer}, device_id_type=MESH,
        )

    def z_refs(c):
        return (ready[c], mid[c]) if c < FIELDS else (early[c - FIELDS], late[c - FIELDS])

    def a_ref(c):
        return placed[c] if c < FIELDS else ready[c]

    def b_ref(c):
        return out_ref.at[c, :, :, span(c)] if c < FIELDS else mid[c]

    def z_copies(c):
        src, dst = z_refs(c)
        return [
            remote(
                src.at[pl.ds(partner(dp, o, n_dp) * m_dp, m_dp)], dst.at[pl.ds(dp * m_dp, m_dp)],
                leave.at[0], z_recv.at[c], "dp", partner(dp, o, n_dp),
            )
            for o in z_order
        ]

    def a_copies(c):
        return [
            remote(
                a_ref(c).at[pl.ds(partner(ep, o, n_ep) * m_ep, m_ep)], e1[c].at[ep],
                leave.at[1], a_recv.at[c], "ep", partner(ep, o, n_ep),
            )
            for o in e_order
        ]

    def b_copies(c):
        return [
            remote(
                sel[c].at[partner(ep, o, n_ep)], b_ref(c).at[pl.ds(ep * m_ep, m_ep)],
                leave.at[2], b_recv.at[c], "ep", partner(ep, o, n_ep),
            )
            for o in e_order
        ]

    def z_all(c):
        src, dst = z_refs(c)
        part = pl.ds(0, (n_dp - 1) * m_dp)
        return remote(src.at[part], dst.at[part], leave.at[0], z_recv.at[c], "dp", partner(dp, 1, n_dp))

    def a_all(c):
        part = pl.ds(0, (n_ep - 1) * m_ep)
        return remote(
            a_ref(c).at[part], e1[c].at[pl.ds(0, n_ep - 1)], leave.at[1], a_recv.at[c], "ep", partner(ep, 1, n_ep)
        )

    def b_all(c):
        part = pl.ds(0, (n_ep - 1) * m_ep)
        return remote(
            sel[c].at[pl.ds(0, n_ep - 1)], b_ref(c).at[part], leave.at[2], b_recv.at[c], "ep", partner(ep, 1, n_ep)
        )

    def start(copies):
        for copy in copies:
            copy.start()

    def make_order():
        def rank_of(e):
            rank = jnp.int32(0)
            for f in range(n_ep):
                tied = (ids_ref[f] == ids_ref[e]) & (f < e)
                rank = rank + ((ids_ref[f] < ids_ref[e]) | tied).astype(I32)
            return rank

        @pl.loop(0, n_ep)
        def _(e):
            rank_ref[e] = rank_of(e)

        @pl.loop(0, n_ep)
        def _(k):
            source = jnp.int32(0)
            for e in range(n_ep):
                source = source + jnp.where(rank_ref[e] == k, e, 0)
            order_ref[k] = source

    def groups_of(writer):
        return (writer == iota((PACK, writer.shape[1]), 0).astype(writer.dtype)).astype(F32)

    def rank_in(groups):
        return dot(groups.astype(BF16), ahead[...])

    def pick(table, s):
        offsets = offsets_ref[:, pl.ds(pl.multiple_of(s * rows, rows), rows)]
        return dot(table, as_bf16(offsets == iota((total, rows), 0)))

    def writer_and_rank(writer):
        groups = groups_of(writer)
        return jnp.sum(groups * rank_in(groups), axis=0, keepdims=True)

    def make_position():
        ahead[...] = as_bf16(iota((rows, rows), 0) < iota((rows, rows), 1))
        picked = pick(stack_rows([writers_ref[...].astype(F32)], total), dp)
        writer = row_of(picked, 0)
        position_ref[...] = (writer * pair + writer_and_rank(writer)).astype(I32)

    def make_targets():
        carry = jnp.zeros((PACK, 1), F32)
        within = []
        for s in range(n_dp):
            groups = groups_of(writers_ref[:, s * rows : (s + 1) * rows])
            count = rank_in(groups) + carry
            carry = carry + jnp.sum(groups, axis=1, keepdims=True)
            within.append(jnp.sum(groups * count, axis=0, keepdims=True).astype(I32))
        place = jnp.concatenate(within, axis=1)
        table = stack_rows(
            [writers_ref[...].astype(F32), (place // 256).astype(F32), (place % 256).astype(F32)], total
        )

        @pl.loop(0, n_dp)
        def _(s):
            picked = pick(table, s)
            writer = row_of(picked, 0)
            here = pl.ds(pl.multiple_of(s * rows, rows), rows)
            target_ref[:, here] = (writer * rows + row_of(picked, 1) * 256 + row_of(picked, 2)).astype(I32)
            arrives_ref[:, here] = (writer_and_rank(writer)).astype(I32) + s * pair

    def after_of(i, j, size):
        return lax.dot_general(
            one_hot(target_ref, dp * rows + i * size, size), one_hot(arrives_ref, j * size, size),
            (((1,), (1,)), ((), ())), preferred_element_type=F32,
        ).astype(BF16)

    permute = functools.partial(permute_rows, aligned)

    def sort(c):
        load_copy(c).wait()

        def body(part):
            x = wide[c][:, part].astype(BF16)
            if aligned:
                ready[c][:, :, part] = dot(before[...], x).astype(BF16).reshape(blocks, depth, part.size)
            else:
                @pl.loop(0, blocks)
                def _(i):
                    ready[c][i, :, part] = dot(one_hot(position_ref, i * depth, depth), x).astype(BF16)

        column_tiles(ready[c].shape[2], body)

    def narrow(c):
        load_copy(c).wait()

        def body(part):
            x = wide[c][:, part].astype(BF16)
            if aligned:
                ready[c][:, :, part] = x.reshape(blocks, depth, part.size)
            else:
                @pl.loop(0, blocks)
                def _(i):
                    keep = as_bf16(iota((depth, rows), 0) + i * depth == iota((depth, rows), 1))
                    ready[c][i, :, part] = dot(keep, x).astype(BF16)

        column_tiles(ready[c].shape[2], body)

    def z_start(c):
        start(z_copies(c))
        src, dst = z_refs(c)
        own = pl.ds(dp * m_dp, m_dp)
        dst[own] = src[own]

    def a_start(c):
        start(a_copies(c))
        e1[c][ep] = a_ref(c)[pl.ds(ep * m_ep, m_ep)]

    def a_to_b(c):
        a_all(c).wait_recv()
        for k in range(n_ep):
            sel[c][k] = e1[c][order_ref[k]]
        start(b_copies(c))
        b_ref(c)[pl.ds(ep * m_ep, m_ep)] = sel[c][ep]

    def z_to_a(c):
        z_all(c).wait_recv()
        permute(after, mid[c], placed[c])
        a_start(c)

    def b_to_z(c):
        b_all(c).wait_recv()
        permute(before, mid[c], early[c - FIELDS])
        z_start(c)

    def finish(c):
        z_all(c).wait_recv()
        permute(after, late[c - FIELDS], out_ref.at[c - FIELDS, :, :, span(c)])

    for copy in index_copies:
        copy.wait()
    make_position()
    if aligned:
        before[...] = one_hot(position_ref, 0, rows)
    sort(0)
    pl.semaphore_wait(barrier, n_dp + n_ep - 2)
    z_start(0)
    narrow(5)
    a_start(5)
    narrow(3)
    a_start(3)
    sort(1)
    z_start(1)
    narrow(4)
    a_start(4)
    sort(2)
    z_start(2)
    make_order()
    make_targets()
    if aligned:
        after[...] = after_of(0, 0, rows)
    else:
        @pl.loop(0, blocks)
        def _(i):
            @pl.loop(0, blocks)
            def _(j):
                after[i, j] = after_of(i, j, depth)
                mine = as_bf16(position_ref[...] == iota((depth, rows), 0) + i * depth)
                whose = as_bf16(iota((depth, rows), 1) == iota((depth, rows), 0) + j * depth)
                before[i, j] = lax.dot_general(
                    mine, whose, (((1,), (1,)), ((), ())), preferred_element_type=F32
                ).astype(BF16)
    a_to_b(3)
    z_to_a(0)
    a_to_b(4)
    a_to_b(5)
    z_to_a(1)
    a_to_b(0)
    b_to_z(3)
    z_to_a(2)
    b_to_z(4)
    b_to_z(5)
    a_to_b(1)
    a_to_b(2)
    finish(3)
    finish(4)
    b_all(0).wait_recv()
    b_all(1).wait_recv()
    z_all(5).wait_recv()
    b_all(2).wait_recv()
    for i, (axis, n, peers) in enumerate((("dp", n_dp, m_dp), ("ep", n_ep, m_ep), ("ep", n_ep, m_ep))):
        part = out_ref.at[:, pl.ds(0, (n - 1) * peers)]
        me = dp if axis == "dp" else ep
        remote(part, part, leave.at[i], z_recv.at[0], axis, partner(me, 1, n)).wait_send()


def exchange(expert_ids, offsets, writers, arrays, n_ep, n_dp):
    rows, cols = arrays[0].shape
    total = offsets.shape[1]
    depth = math.gcd(rows // n_dp, rows // n_ep)
    blocks = rows // depth
    split = widths(cols)
    per = blocks // n_ep
    size = split + [cols - w for w in split]
    dma = pltpu.SemaphoreType.DMA
    vmem = pl.BlockSpec(memory_space=pltpu.VMEM)
    square = (rows, rows) if depth % PACK == 0 else (blocks, blocks, depth, depth)

    def each(shape, widths_of, kind=BF16):
        return [pltpu.VMEM((*shape, w), kind) for w in widths_of]

    first, last = size[:FIELDS], size[FIELDS:]
    chunks = 2 * FIELDS
    most, late, after = pl.pallas_call(
        functools.partial(exchange_kernel, n_ep, n_dp, split),
        out_shape=[
            pltpu.VMEM((FIELDS, blocks, depth, cols), BF16),
            pltpu.VMEM((blocks, depth, last[-1]), BF16),
            pltpu.VMEM(square, BF16),
        ],
        in_specs=[pl.BlockSpec(memory_space=pl.ANY)] * (3 + FIELDS),
        out_specs=[vmem] * 3,
        scratch_shapes=each((rows,), size, F32)
        + each((blocks, depth), size)
        + each((blocks, depth), size)
        + each((n_ep, per, depth), size)
        + each((n_ep, per, depth), size)
        + each((blocks, depth), first)
        + each((blocks, depth), last)
        + each((blocks, depth), last[:-1])
        + [
            pltpu.SMEM((n_ep,), I32),
            pltpu.VMEM((1, total), I32),
            pltpu.VMEM((1, total), I32),
            pltpu.SMEM((n_ep,), I32),
            pltpu.SMEM((n_ep,), I32),
            pltpu.VMEM((1, rows), I32),
            pltpu.VMEM((1, total), I32),
            pltpu.VMEM((1, total), I32),
            pltpu.VMEM(square, BF16),
            pltpu.VMEM((rows, rows), BF16),
            dma((chunks,)),
            dma((3,)),
            dma((chunks,)),
            dma((chunks,)),
            dma((chunks,)),
            dma((3,)),
        ],
        compiler_params=pltpu.CompilerParams(
            collective_id=0, has_side_effects=True, vmem_limit_bytes=54 * 2**20
        ),
    )(expert_ids, offsets, writers, *arrays)
    in_vmem = [pltpu.with_memory_space_constraint(x, pltpu.VMEM) for x in (most, late, after)]
    return pl.pallas_call(
        functools.partial(last_kernel, split),
        out_shape=jax.ShapeDtypeStruct((FIELDS, blocks, depth, cols), BF16),
        in_specs=[vmem] * 3,
        out_specs=pl.BlockSpec(memory_space=pl.ANY),
        scratch_shapes=[pltpu.VMEM((blocks, depth, last[-1]), BF16), dma((FIELDS + 1, 1))],
        compiler_params=pltpu.CompilerParams(vmem_limit_bytes=8 * 2**20),
    )(*in_vmem)


def on_device(master_weights, first_moment, second_moment, expert_ids, bucket_offsets, writer_rank):
    n_dp, n_ep = lax.axis_size("dp"), lax.axis_size("ep")
    _, rows, cols = master_weights.shape
    total = bucket_offsets.shape[0]
    arrays = (master_weights[0], first_moment[0], second_moment[0])
    saved = exchange(
        expert_ids, bucket_offsets.reshape(1, total), writer_rank.reshape(1, total), arrays, n_ep, n_dp
    )
    return saved.reshape(FIELDS, 1, rows, cols)


def solution(mesh):
    return jax.shard_map(
        on_device,
        mesh=mesh,
        in_specs=(P("ep", "dp", None), P("ep", "dp", None), P("ep", "dp", None), P(), P(), P()),
        out_specs=P(None, "ep", "dp", None),
        check_vma=False,
    )
```
